128 devices in a mesh: lat: 32 (over x, y, core), lon: 4 (over z).
Axes of the slice: x: 4, y: 4, z: 4, core: 2. Of those that a mesh axis runs over, the one named last changes fastest.
Arguments:
- coeffs_old: float32 [640, 2, 3, 50, 640], P(('lat', 'lon')), may hold values from -0.16 to 0.16
- noise: bfloat16 [640, 2, 3, 50, 640], P(('lat', 'lon')), may hold values from -6 to 6
- legendre: float32 [640, 640, 640], P(('lat', 'lon')), may hold values from -0.25 to 0.25
- decay: float32 [3], replicated, may hold values from 0.3 to 0.97
- amplitude: float32 [3, 640], replicated, may hold values from 0.005 to 0.05
- wavenumber_of_slot: int32 [640], replicated, may hold values from 0 to 639, as said below
- lat_order: int32 [640], replicated, may hold values from 0 to 639, each once
Outputs:
- coeffs_new: float32 [640, 2, 3, 50, 640], P(('lat', 'lon'))
- pattern: float32 [640, 50, 1280], P(('lat', 'lon'))
The draws below stay inside these ranges and needn't reach their ends.
Inputs may be any that keep to these rules, and one draw needn't show every extreme that they name: `wavenumber_of_slot`: every wavenumber fills exactly one slot; the sums of the wavenumbers of one device's 5 slots differ between devices by less than 128. `lat_order`: every latitude stands in exactly one row.
All inputs are finite; a program needn't handle non-finite values.
Results may differ from the reference program's by a relative error of at most 0.0003.
Values sent between devices are 32-bit elements; how exact they have to be, the bound alone decides.
A program may use at most 128 MiB of HBM per device.

```python
import math
import jax
import jax.numpy as jnp
from jax import lax

M = 640
LAT = 640
LON = 1280
SCALES = 3
MEMBERS = 50
SLOT_DEV = 5


def draw_wavenumber_of_slot(key, part):
    devices_all = M // SLOT_DEV
    position = jax.random.permutation(jax.random.fold_in(key, 11), devices_all).astype(jnp.int32)
    rounds = jnp.arange(SLOT_DEV, dtype=jnp.int32)
    dealt = jnp.where(rounds[None, :] % 2 == 0, position[:, None], devices_all - 1 - position[:, None])
    table = rounds[None, :] * devices_all + dealt
    return table.reshape(-1).astype(jnp.int32)


def shard_levels(stream_key, shape, cuts, low, high):
    def one(dim, blocks):
        steps = jax.random.uniform(jax.random.fold_in(jax.random.fold_in(stream_key, 6), dim), (blocks,), jnp.float32, low / len(cuts), high / len(cuts))
        return jnp.repeat(jnp.exp(steps), shape[dim] // blocks).reshape((-1,) + (1,) * (len(shape) - dim - 1))

    loudness = one(*cuts[0])
    for cut in cuts[1:]:
        loudness = loudness * one(*cut)
    return loudness


def scatter_about(own_key, dims, scale, bound, shards=(), kind=jnp.bfloat16):
    result = scale * jax.random.normal(own_key, dims, jnp.float32)
    if shards:
        result = result * shard_levels(own_key, dims, shards, -0.22, 0.18)
    return jnp.clip(result, -bound, bound).astype(kind)


def setup_inputs(seed: int = 0) -> dict:
    arg_keys = jax.random.split(jax.random.key(seed), 8)
    coeffs_old = scatter_about(arg_keys[0], (M, 2, SCALES, MEMBERS, M), 0.02, 0.16, ((0, 128),), jnp.float32)
    noise = scatter_about(arg_keys[1], (M, 2, SCALES, MEMBERS, M), 1.0, 6.0, ((0, 128),))
    legendre = scatter_about(arg_keys[2], (M, LAT, M), M ** -0.5, 0.25, ((0, 128),), jnp.float32)
    decay = jnp.clip(jax.random.uniform(arg_keys[3], (SCALES,), jnp.float32, 0.3, 0.97), 0.3, 0.97)
    amplitude = jnp.clip(jnp.exp(jax.random.uniform(arg_keys[4], (SCALES, M), jnp.float32, math.log(0.005), math.log(0.05))), 0.005, 0.05)
    wavenumber_of_slot = draw_wavenumber_of_slot(jax.random.fold_in(arg_keys[7], 71), 0)
    lat_order = jax.random.permutation(arg_keys[6], LAT).astype(jnp.int32)
    return {"coeffs_old": coeffs_old, "noise": noise, "legendre": legendre, "decay": decay, "amplitude": amplitude, "wavenumber_of_slot": wavenumber_of_slot, "lat_order": lat_order}


def evolve(coeffs_old, noise, decay, amplitude, waves):
    width = coeffs_old.shape[4]
    offsets = lax.broadcasted_iota(jnp.int32, (waves.shape[0], width), 1)
    live = waves[:, None] + offsets < width
    padded = jnp.concatenate([amplitude, jnp.zeros_like(amplitude)], axis=1)
    spread = jax.vmap(lambda wave: lax.dynamic_slice_in_dim(padded, wave, width, 1))(waves)
    factor = jnp.sqrt(1.0 - decay * decay)
    fresh = decay[None, None, :, None, None] * coeffs_old + (spread * factor[None, :, None])[:, None, :, None, :] * noise.astype(jnp.float32)
    return jnp.where(live[:, None, None, None, :], fresh, jnp.zeros_like(fresh))

def reference(coeffs_old, noise, legendre, decay, amplitude, wavenumber_of_slot, lat_order):
    waves = wavenumber_of_slot.astype(jnp.int32)
    coeffs_new = evolve(coeffs_old, noise, decay, amplitude, waves)

    def per_slot(pair):
        coeff, basis = pair
        return jnp.einsum('rkej,lj->rel', coeff, basis, precision=lax.Precision.HIGHEST)
    field = lax.map(per_slot, (coeffs_new, legendre))
    real_part = jnp.zeros((M,) + field.shape[2:], field.dtype).at[waves].set(field[:, 0])
    imag_part = jnp.zeros((M,) + field.shape[2:], field.dtype).at[waves].set(field[:, 1])
    positive = jnp.arange(M, dtype=jnp.int32)[:, None, None] > 0
    imag_part = jnp.where(positive, imag_part, jnp.zeros_like(imag_part))
    real_part = jnp.take(real_part, lat_order.astype(jnp.int32), axis=2)
    imag_part = jnp.take(imag_part, lat_order.astype(jnp.int32), axis=2)
    spectrum = real_part + 1j * imag_part
    grid = jnp.fft.irfft(spectrum, n=LON, axis=0) * LON
    pattern = jnp.transpose(grid, (2, 1, 0))
    return (coeffs_new, pattern)
```

```python
import functools

import jax
import jax.numpy as jnp
from jax import lax
from jax.experimental import pallas as pl
from jax.experimental.pallas import tpu as pltpu
from jax.sharding import PartitionSpec as P

MESH = pl.DeviceIdType.MESH
LON = 1280
HALF = LON // 2
TWO_PI = 6.283185307179586
SLOTS = 5
DEVS = 128
ROWS = 5
MEMBERS = 50
WIDTH = 640
SCALES = 3
F32 = jnp.float32
BF16 = jnp.bfloat16


def evolve_kernel(waves_ref, decay_ref, amp_ref, old_ref, noise_ref, new_ref, sum_ref):
    s = pl.program_id(0)
    me = lax.axis_index("lat") * 4 + lax.axis_index("lon")
    wave = waves_ref[me * SLOTS + s]
    lane = lax.broadcasted_iota(jnp.int32, (1, WIDTH), 1)
    live = lane < WIDTH - wave
    shifted = pltpu.roll(amp_ref[...], lax.rem(WIDTH - wave, WIDTH), 1)
    keep, gain = [], []
    for k in range(SCALES):
        d = jnp.full((1, WIDTH), decay_ref[k], F32)
        keep.append(jnp.where(live, d, 0.0))
        gain.append(jnp.where(live, shifted[k : k + 1] * jnp.sqrt(1.0 - d * d), 0.0))
    for e in range(MEMBERS):
        total = None
        for k in range(SCALES):
            fresh = keep[k] * old_ref[0, k, e] + gain[k] * noise_ref[0, k, e].astype(F32)
            new_ref[0, k, e] = fresh
            total = fresh if total is None else total + fresh
        sum_ref[0, e : e + 1, :] = total[0:1]
        sum_ref[0, MEMBERS + e : MEMBERS + e + 1, :] = total[1:2]


def evolve(waves, decay, amplitude, old, noise):
    block = pl.BlockSpec((1, SCALES, MEMBERS, 2, WIDTH), lambda s: (s, 0, 0, 0, 0))
    return pl.pallas_call(
        evolve_kernel,
        name="evolve",
        grid=(SLOTS,),
        out_shape=(
            jax.ShapeDtypeStruct((SLOTS, SCALES, MEMBERS, 2, WIDTH), F32),
            jax.ShapeDtypeStruct((SLOTS, 2 * MEMBERS, WIDTH), F32),
        ),
        in_specs=[
            pl.BlockSpec(memory_space=pltpu.SMEM),
            pl.BlockSpec(memory_space=pltpu.SMEM),
            pl.BlockSpec(memory_space=pltpu.VMEM),
            block,
            block,
        ],
        out_specs=(block, pl.BlockSpec((1, 2 * MEMBERS, WIDTH), lambda s: (s, 0, 0))),
        compiler_params=pltpu.CompilerParams(dimension_semantics=("arbitrary",)),
    )(waves, decay, amplitude, old, noise)


def offsets():
    out = []
    for dx in range(4):
        for dy in range(4):
            for dz in range(4):
                for dc in range(2):
                    if dx or dy or dz or dc:
                        hops = sum(min(d, 4 - d) for d in (dx, dy, dz))
                        out.append((-hops, dx, dy, dz, dc))
    return [o[1:] for o in sorted(out)]


def split(x):
    hi = x.astype(BF16)
    return hi, (x - hi.astype(F32)).astype(BF16)


def dot(a, b, dims=(((1,), (0,)), ((), ()))):
    return lax.dot_general(a, b, dims, preferred_element_type=F32)


def unit(turns):
    near = jnp.round(turns * (1.0 / LON))
    x = (turns - near * LON) * (TWO_PI / LON)
    y = x * x
    c, s = None, None
    for n in range(8, -1, -1):
        a = (-1.0) ** n
        fact = 1.0
        for i in range(1, 2 * n + 1):
            fact *= i
        c = a / fact if c is None else c * y + a / fact
        s = a / (fact * (2 * n + 1)) if s is None else s * y + a / (fact * (2 * n + 1))
    return c, s * x


def exchange_kernel(
    order_ref, waves_ref, sum_hbm, leg_hbm, out_ref,
    coef, leg, perm, send, recv, tab_hi, tab_lo, acc,
    coef_sem, leg_sem, send_sem, recv_sem,
):
    lat = lax.axis_index("lat")
    z = lax.axis_index("lon")
    me = lat * 4 + z
    x, y, c = lat // 8, lax.rem(lat // 2, 4), lax.rem(lat, 2)

    def peer(o):
        dx, dy, dz, dc = o
        px, py, pz = lax.rem(x + dx, 4), lax.rem(y + dy, 4), lax.rem(z + dz, 4)
        pc = lax.rem(c + dc, 2)
        return (px * 4 + py) * 2 + pc, pz

    barrier = pltpu.get_barrier_semaphore()
    peers = [peer(o) for o in offsets()]
    for p in peers:
        pl.semaphore_signal(barrier, inc=1, device_id=p, device_id_type=MESH)
    loads = []
    for s in range(SLOTS):
        a = pltpu.make_async_copy(sum_hbm.at[s], coef.at[s], coef_sem.at[s])
        b = pltpu.make_async_copy(leg_hbm.at[s], leg.at[s], leg_sem.at[s])
        a.start()
        b.start()
        loads.append((a, b))

    lane = lax.broadcasted_iota(jnp.int32, (DEVS, WIDTH), 1)
    row = lax.broadcasted_iota(jnp.int32, (DEVS, WIDTH), 0)
    order = order_ref[...]
    for q in range(ROWS):
        mine = jnp.where(lane == row * ROWS + q, order, 0)
        shown = jnp.sum(mine.astype(F32), axis=1, keepdims=True).astype(jnp.int32)
        perm[q * DEVS : (q + 1) * DEVS, :] = jnp.where(lane == shown, 1.0, 0.0).astype(BF16)

    lanes = lax.broadcasted_iota(jnp.int32, (DEVS, 128), 1)
    nt = (((1,), (1,)), ((), ()))

    def field(s):
        for copy in loads[s]:
            copy.wait()
        c_hi, c_lo = split(coef[s])
        pad = jnp.zeros((128 - 2 * MEMBERS, WIDTH), BF16)
        c_hi = jnp.concatenate([c_hi, pad], axis=0)
        c_lo = jnp.concatenate([c_lo, pad], axis=0)
        l_hi, l_lo = split(leg[s])
        f = dot(l_hi, c_hi, nt) + (dot(l_hi, c_lo, nt) + dot(l_lo, c_hi, nt))
        f_hi, f_lo = split(f)
        p = perm[...]
        g = dot(p, f_hi) + dot(p, f_lo)
        for r in range(2):
            low, high = None, None
            for q in range(ROWS):
                block = g[q * DEVS : (q + 1) * DEVS]
                shift = ((q - r) * MEMBERS) % 128
                if shift:
                    block = pltpu.roll(block, shift, 1)
                start = q * MEMBERS
                if start < 128:
                    low = block if low is None else jnp.where(lanes >= start, block, low)
                if start + MEMBERS > 128:
                    high = block if high is None else jnp.where(lanes >= start - 128, block, high)
            send[s, :, 2 * r, :] = low
            send[s, :, 2 * r + 1, :] = high

    def start(s):
        for p in peers:
            pltpu.make_async_remote_copy(
                src_ref=send.at[s, p[0] * 4 + p[1]],
                dst_ref=recv.at[s, me],
                send_sem=send_sem.at[s],
                recv_sem=recv_sem.at[s],
                device_id=p,
                device_id_type=MESH,
            ).start()
        recv[s, pl.ds(me, 1)] = send[s, pl.ds(me, 1)]

    field(0)
    pl.semaphore_wait(barrier, DEVS - 1)
    start(0)
    for s in range(1, SLOTS):
        field(s)
        start(s)

    waves = waves_ref[...]
    signs = []
    for s in range(SLOTS):
        mine = jnp.where(lane == row * SLOTS + s, waves, 0)
        m = jnp.sum(mine.astype(F32), axis=1, keepdims=True)
        m = jnp.broadcast_to(m, (DEVS, 128))
        weight = jnp.where(m == 0.0, 1.0, 2.0)
        cos, sin = unit(m * lanes.astype(F32))
        step_c, step_s = unit(m * 128.0)
        cos, sin = weight * cos, -weight * sin
        for a in range(HALF // 128):
            hi, lo = split(cos)
            tab_hi[s, 0:DEVS, a * 128 : (a + 1) * 128] = hi
            tab_lo[s, 0:DEVS, a * 128 : (a + 1) * 128] = lo
            hi, lo = split(sin)
            tab_hi[s, DEVS:, a * 128 : (a + 1) * 128] = hi
            tab_lo[s, DEVS:, a * 128 : (a + 1) * 128] = lo
            cos, sin = cos * step_c + sin * step_s, sin * step_c - cos * step_s
        odd = m - 2.0 * jnp.floor(m * 0.5)
        sign = (1.0 - 2.0 * odd).T
        signs.append(jnp.concatenate([sign[0:1], sign[0:1]], axis=1).astype(F32))

    for s in range(SLOTS):
        whole = recv.at[s, pl.ds(0, DEVS - 1)]
        pltpu.make_async_copy(whole, whole, recv_sem.at[s]).wait()
        rows = []
        for lt in range(2):
            got = jnp.concatenate([recv[s, :, 2 * r + lt, :] for r in range(2)], axis=0)
            rows.append(got.T)
        w = jnp.concatenate(rows, axis=0)
        w_hi, w_lo = split(w)
        sg = signs[s].astype(BF16)
        left_hi = jnp.concatenate([w_hi, w_hi * sg], axis=0)
        left_lo = jnp.concatenate([w_lo, w_lo * sg], axis=0)
        t_hi, t_lo = tab_hi[s], tab_lo[s]
        part = dot(left_hi, t_hi) + (dot(left_lo, t_hi) + dot(left_hi, t_lo))
        if s == 0:
            acc[...] = part
        else:
            acc[...] += part
    for q in range(ROWS):
        for h in range(2):
            base = h * 256 + q * MEMBERS
            out_ref[q, :, h * HALF : (h + 1) * HALF] = acc[base : base + MEMBERS, :]
    for s in range(SLOTS):
        whole = send.at[s, pl.ds(0, DEVS - 1)]
        pltpu.make_async_copy(whole, whole, send_sem.at[s]).wait()


def exchange(order, waves, summed, legendre):
    return pl.pallas_call(
        exchange_kernel,
        name="exchange",
        out_shape=jax.ShapeDtypeStruct((ROWS, MEMBERS, LON), F32),
        in_specs=[
            pl.BlockSpec(memory_space=pltpu.VMEM),
            pl.BlockSpec(memory_space=pltpu.VMEM),
            pl.BlockSpec(memory_space=pl.ANY),
            pl.BlockSpec(memory_space=pl.ANY),
        ],
        out_specs=pl.BlockSpec(memory_space=pltpu.VMEM),
        scratch_shapes=[
            pltpu.VMEM((SLOTS, 2 * MEMBERS, WIDTH), F32),
            pltpu.VMEM((SLOTS, WIDTH, WIDTH), F32),
            pltpu.VMEM((WIDTH, WIDTH), BF16),
            pltpu.VMEM((SLOTS, DEVS, 4, 128), F32),
            pltpu.VMEM((SLOTS, DEVS, 4, 128), F32),
            pltpu.VMEM((SLOTS, 2 * DEVS, HALF), BF16),
            pltpu.VMEM((SLOTS, 2 * DEVS, HALF), BF16),
            pltpu.VMEM((512, HALF), F32),
            pltpu.SemaphoreType.DMA((SLOTS,)),
            pltpu.SemaphoreType.DMA((SLOTS,)),
            pltpu.SemaphoreType.DMA((SLOTS,)),
            pltpu.SemaphoreType.DMA((SLOTS,)),
        ],
        compiler_params=pltpu.CompilerParams(collective_id=0, has_side_effects=True, vmem_limit_bytes=48 * 2**20),
    )(order, waves, summed, legendre)


def local(coeffs_old, noise, legendre, decay, amplitude, wavenumber_of_slot, lat_order):
    old = coeffs_old.transpose(0, 2, 3, 1, 4)
    fresh = noise.transpose(0, 2, 3, 1, 4)
    new, summed = evolve(wavenumber_of_slot, decay, amplitude, old, fresh)
    pattern = exchange(lat_order.reshape(1, -1), wavenumber_of_slot.reshape(1, -1), summed, legendre)
    return new.transpose(0, 3, 1, 2, 4), pattern


def solution(mesh):
    split_slots = P(("lat", "lon"), None, None, None, None)
    in_specs = (split_slots, split_slots, P(("lat", "lon"), None, None), P(), P(), P(), P())
    out_specs = (split_slots, P(("lat", "lon"), None, None))
    return jax.shard_map(local, mesh=mesh, in_specs=in_specs, out_specs=out_specs, check_vma=False)
```

```python
import functools

import jax
import jax.numpy as jnp
from jax import lax
from jax.experimental import pallas as pl
from jax.experimental.pallas import tpu as pltpu
from jax.sharding import PartitionSpec as P

MESH = pl.DeviceIdType.MESH
LON = 1280
HALF = LON // 2
TWO_PI = 6.283185307179586
SLOTS = 5
DEVS = 128
ROWS = 5
MEMBERS = 50
WIDTH = 640
SCALES = 3
TILES = WIDTH // 128
F32 = jnp.float32
BF16 = jnp.bfloat16


def offsets():
    out = []
    for dx in range(4):
        for dy in range(4):
            for dz in range(4):
                for dc in range(2):
                    if dx or dy or dz or dc:
                        hops = sum(min(d, 4 - d) for d in (dx, dy, dz))
                        out.append((-hops, dx, dy, dz, dc))
    return [o[1:] for o in sorted(out)]


def split(x):
    hi = x.astype(BF16)
    return hi, (x - hi.astype(F32)).astype(BF16)


def dot(a, b, dims=(((1,), (0,)), ((), ()))):
    return lax.dot_general(a, b, dims, preferred_element_type=F32)


def unit(turns):
    near = jnp.round(turns * (1.0 / LON))
    x = (turns - near * LON) * (TWO_PI / LON)
    y = x * x
    c, s = None, None
    for n in range(8, -1, -1):
        a = (-1.0) ** n
        fact = 1.0
        for i in range(1, 2 * n + 1):
            fact *= i
        c = a / fact if c is None else c * y + a / fact
        s = a / (fact * (2 * n + 1)) if s is None else s * y + a / (fact * (2 * n + 1))
    return c, s * x


def exchange_kernel(
    order_hbm, waves_hbm, decay_hbm, amp_hbm, old_hbm, noise_hbm, leg_hbm,
    new_ref, acc_ref, last_ref, sign_ref, last_hi, last_lo,
    order_ref, waves_ref, wave_ref, decay_ref, amp_ref,
    old, noise, leg, total, coef, perm, send, recv, tab_hi, tab_lo,
    small_sem, load_sem, leg_sem, send_sem, recv_sem,
):
    lat = lax.axis_index("lat")
    z = lax.axis_index("lon")
    me = lat * 4 + z
    x, y, c = lat // 8, lax.rem(lat // 2, 4), lax.rem(lat, 2)

    def peer(o):
        dx, dy, dz, dc = o
        px, py, pz = lax.rem(x + dx, 4), lax.rem(y + dy, 4), lax.rem(z + dz, 4)
        pc = lax.rem(c + dc, 2)
        return (px * 4 + py) * 2 + pc, pz

    barrier = pltpu.get_barrier_semaphore()
    peers = [peer(o) for o in offsets()]
    for p in peers:
        pl.semaphore_signal(barrier, inc=1, device_id=p, device_id_type=MESH)

    def load(s):
        for t in range(TILES):
            lanes_of = pl.ds(t * 128, 128)
            pltpu.make_async_copy(old_hbm.at[s, :, :, :, lanes_of], old.at[s, t], load_sem.at[0, s]).start()
            pltpu.make_async_copy(noise_hbm.at[s, :, :, :, lanes_of], noise.at[s, t], load_sem.at[1, s]).start()
        pltpu.make_async_copy(leg_hbm.at[s], leg.at[s], leg_sem.at[s]).start()

    small = [
        pltpu.make_async_copy(src, dst, small_sem.at[i])
        for i, (src, dst) in enumerate(
            [
                (order_hbm, order_ref),
                (waves_hbm, waves_ref),
                (waves_hbm, wave_ref),
                (decay_hbm, decay_ref),
                (amp_hbm, amp_ref),
            ]
        )
    ]
    for copy in small:
        copy.start()
    load(0)
    load(1)
    for copy in small:
        copy.wait()

    lane = lax.broadcasted_iota(jnp.int32, (DEVS, WIDTH), 1)
    row = lax.broadcasted_iota(jnp.int32, (DEVS, WIDTH), 0)
    order = order_ref[...].reshape(1, WIDTH)
    for q in range(ROWS):
        mine = jnp.where(lane == row * ROWS + q, order, 0)
        shown = jnp.sum(mine.astype(F32), axis=1, keepdims=True).astype(jnp.int32)
        perm[q * DEVS : (q + 1) * DEVS, :] = jnp.where(lane == shown, 1.0, 0.0).astype(BF16)

    lanes = lax.broadcasted_iota(jnp.int32, (DEVS, 128), 1)
    nt = (((1,), (1,)), ((), ()))
    amp = amp_ref[...]
    coef[...] = jnp.zeros_like(coef)

    def advance(s):
        pltpu.make_async_copy(old.at[s], old.at[s], load_sem.at[0, s]).wait()
        pltpu.make_async_copy(noise.at[s], noise.at[s], load_sem.at[1, s]).wait()
        wave = wave_ref[me * SLOTS + s]
        live = lane[0:1] < WIDTH - wave
        shifted = pltpu.roll(amp, lax.rem(WIDTH - wave, WIDTH), 1)
        keep, gain = [], []
        for k in range(SCALES):
            d = jnp.full((1, WIDTH), decay_ref[k], F32)
            keep.append(jnp.where(live, d, 0.0))
            gain.append(jnp.where(live, shifted[k : k + 1] * jnp.sqrt(1.0 - d * d), 0.0))
        for t in range(TILES):
            at = slice(t * 128, (t + 1) * 128)
            summed = None
            for k in range(SCALES):
                fresh = (
                    keep[k][:, at] * old.at[s, t, k].reshape(2 * MEMBERS, 128)[...]
                    + gain[k][:, at] * noise.at[s, t, k].reshape(2 * MEMBERS, 128)[...].astype(F32)
                )
                new_ref.at[s, t, k].reshape(2 * MEMBERS, 128)[...] = fresh
                summed = fresh if summed is None else summed + fresh
            total[t, 0 : 2 * MEMBERS, :] = summed
            for r in range(2):
                coef[r * 64 : r * 64 + MEMBERS, at] = total[t, pl.ds(r, MEMBERS, stride=2), :]

    def field(s):
        advance(s)
        pltpu.make_async_copy(leg_hbm.at[s], leg.at[s], leg_sem.at[s]).wait()
        if s + 2 < SLOTS:
            load(s + 2)
        c_hi, c_lo = split(coef[...])
        l_hi, l_lo = split(leg[s])
        f = dot(l_hi, jnp.concatenate([c_hi, c_lo], axis=0), nt)
        f = f[:, 0:128] + (f[:, 128:] + dot(l_lo, c_hi, nt))
        f_hi, f_lo = split(f)
        g = dot(perm[...], jnp.concatenate([f_hi, f_lo], axis=1))
        g = g[:, 0:128] + g[:, 128:]
        for r in range(2):
            low, high = None, None
            for q in range(ROWS):
                block = g[q * DEVS : (q + 1) * DEVS]
                shift = (q * MEMBERS - r * 64) % 128
                if shift:
                    block = pltpu.roll(block, shift, 1)
                start = q * MEMBERS
                if start < 128:
                    low = block if low is None else jnp.where(lanes >= start, block, low)
                if start + MEMBERS > 128:
                    high = block if high is None else jnp.where(lanes >= start - 128, block, high)
            send[s, :, 2 * r, :] = low
            send[s, :, 2 * r + 1, :] = high

    def start(s):
        for p in peers:
            pltpu.make_async_remote_copy(
                src_ref=send.at[s, p[0] * 4 + p[1]],
                dst_ref=recv.at[s, me],
                send_sem=send_sem.at[s],
                recv_sem=recv_sem.at[s],
                device_id=p,
                device_id_type=MESH,
            ).start()
        recv[s, pl.ds(me, 1)] = send[s, pl.ds(me, 1)]

    field(0)
    pl.semaphore_wait(barrier, DEVS - 1)
    start(0)
    for s in range(1, SLOTS):
        field(s)
        start(s)

    waves = waves_ref[...].reshape(1, WIDTH)
    signs = []
    for s in range(SLOTS):
        if s < SLOTS - 1:
            t_hi, t_lo = tab_hi.at[s], tab_lo.at[s]
        else:
            t_hi, t_lo = last_hi, last_lo
        mine = jnp.where(lane == row * SLOTS + s, waves, 0)
        m = jnp.sum(mine.astype(F32), axis=1, keepdims=True)
        m = jnp.broadcast_to(m, (DEVS, 128))
        weight = jnp.where(m == 0.0, 1.0, 2.0)
        cos, sin = unit(m * lanes.astype(F32))
        step_c, step_s = unit(m * 128.0)
        cos, sin = weight * cos, -weight * sin
        for a in range(HALF // 128):
            at = slice(a * 128, (a + 1) * 128)
            t_hi[0:DEVS, at], t_lo[0:DEVS, at] = split(cos)
            t_hi[DEVS:, at], t_lo[DEVS:, at] = split(sin)
            cos, sin = cos * step_c + sin * step_s, sin * step_c - cos * step_s
        odd = m - 2.0 * jnp.floor(m * 0.5)
        sign = (1.0 - 2.0 * odd).T
        signs.append(jnp.concatenate([sign[0:8], sign[0:8]], axis=1))
    sign_ref[...] = signs[SLOTS - 1]

    for s in range(SLOTS):
        whole = recv.at[s, pl.ds(0, DEVS - 1)]
        pltpu.make_async_copy(whole, whole, recv_sem.at[s]).wait()
        rows = []
        for lt in range(2):
            got = jnp.concatenate([recv[s, :, 2 * r + lt, :] for r in range(2)], axis=0)
            rows.append(got.T)
        w = jnp.concatenate(rows, axis=0)
        if s == SLOTS - 1:
            last_ref[...] = w
        elif s == 0:
            acc_ref[...] = synthesize(w, signs[s], tab_hi[s], tab_lo[s])
        else:
            acc_ref[...] += synthesize(w, signs[s], tab_hi[s], tab_lo[s])
    for s in range(SLOTS):
        whole = send.at[s, pl.ds(0, DEVS - 1)]
        pltpu.make_async_copy(whole, whole, send_sem.at[s]).wait()


def synthesize(w, sign, t_hi, t_lo):
    w_hi, w_lo = split(w)
    sg = sign[0:1].astype(BF16)
    left_hi = jnp.concatenate([w_hi, w_hi * sg], axis=0)
    left_lo = jnp.concatenate([w_lo, w_lo * sg], axis=0)
    return dot(jnp.concatenate([left_hi, left_lo], axis=0), t_hi).reshape(2, 512, HALF).sum(0) + dot(left_hi, t_lo)


def finish_kernel(new_ref, acc_ref, last_ref, sign_ref, last_hi, last_lo, new_hbm, out_hbm, out, new_sem, out_sem):
    for s in range(SLOTS):
        for t in range(TILES):
            pltpu.make_async_copy(
                new_ref.at[s, t], new_hbm.at[s, :, :, :, pl.ds(t * 128, 128)], new_sem.at[s]
            ).start()
    both = acc_ref[...] + synthesize(last_ref[...], sign_ref[...], last_hi[...], last_lo[...])
    for q in range(ROWS):
        for h in range(2):
            base = h * 256 + q * MEMBERS
            out[q, :, h * HALF : (h + 1) * HALF] = both[base : base + MEMBERS, :]
        pltpu.make_async_copy(out.at[q], out_hbm.at[q], out_sem.at[q]).start()
    for q in range(ROWS):
        pltpu.make_async_copy(out.at[q], out_hbm.at[q], out_sem.at[q]).wait()
    for s in range(SLOTS):
        pltpu.make_async_copy(new_ref.at[s], new_ref.at[s], new_sem.at[s]).wait()


def local(coeffs_old, noise, legendre, decay, amplitude, wavenumber_of_slot, lat_order):
    old = coeffs_old.transpose(0, 2, 3, 1, 4)
    fresh = noise.transpose(0, 2, 3, 1, 4)
    vmem = pl.BlockSpec(memory_space=pltpu.VMEM)
    hbm = pl.BlockSpec(memory_space=pltpu.HBM)
    block = (SLOTS, TILES, SCALES, MEMBERS, 2, 128)
    kept = pl.pallas_call(
        exchange_kernel,
        name="exchange",
        out_shape=(
            pltpu.VMEM(block, F32),
            pltpu.VMEM((512, HALF), F32),
            pltpu.VMEM((256, 256), F32),
            pltpu.VMEM((8, 256), F32),
            pltpu.VMEM((2 * DEVS, HALF), BF16),
            pltpu.VMEM((2 * DEVS, HALF), BF16),
        ),
        in_specs=[hbm] * 7,
        out_specs=(vmem,) * 6,
        scratch_shapes=[
            pltpu.VMEM((WIDTH,), jnp.int32),
            pltpu.VMEM((WIDTH,), jnp.int32),
            pltpu.SMEM((WIDTH,), jnp.int32),
            pltpu.SMEM((SCALES,), F32),
            pltpu.VMEM((SCALES, WIDTH), F32),
            pltpu.VMEM(block, F32),
            pltpu.VMEM(block, BF16),
            pltpu.VMEM((SLOTS, WIDTH, WIDTH), F32),
            pltpu.VMEM((TILES, 104, 128), F32),
            pltpu.VMEM((128, WIDTH), F32),
            pltpu.VMEM((WIDTH, WIDTH), BF16),
            pltpu.VMEM((SLOTS, DEVS, 4, 128), F32),
            pltpu.VMEM((SLOTS, DEVS, 4, 128), F32),
            pltpu.VMEM((SLOTS - 1, 2 * DEVS, HALF), BF16),
            pltpu.VMEM((SLOTS - 1, 2 * DEVS, HALF), BF16),
            pltpu.SemaphoreType.DMA((5,)),
            pltpu.SemaphoreType.DMA((2, SLOTS)),
            pltpu.SemaphoreType.DMA((SLOTS,)),
            pltpu.SemaphoreType.DMA((SLOTS,)),
            pltpu.SemaphoreType.DMA((SLOTS,)),
        ],
        compiler_params=pltpu.CompilerParams(collective_id=0, has_side_effects=True, vmem_limit_bytes=44 * 2**20),
    )(*(pltpu.with_memory_space_constraint(v, pltpu.HBM) for v in (lat_order, wavenumber_of_slot, decay, amplitude, old, fresh, legendre)))
    new, pattern = pl.pallas_call(
        finish_kernel,
        name="finish",
        out_shape=(
            jax.ShapeDtypeStruct((SLOTS, SCALES, MEMBERS, 2, WIDTH), F32),
            jax.ShapeDtypeStruct((ROWS, MEMBERS, LON), F32),
        ),
        in_specs=[vmem] * 6,
        out_specs=(hbm, hbm),
        scratch_shapes=[
            pltpu.VMEM((ROWS, MEMBERS, LON), F32),
            pltpu.SemaphoreType.DMA((SLOTS,)),
            pltpu.SemaphoreType.DMA((ROWS,)),
        ],
        compiler_params=pltpu.CompilerParams(vmem_limit_bytes=24 * 2**20),
    )(*kept)
    return new.transpose(0, 3, 1, 2, 4), pattern


def solution(mesh):
    split_slots = P(("lat", "lon"), None, None, None, None)
    in_specs = (split_slots, split_slots, P(("lat", "lon"), None, None), P(), P(), P(), P())
    out_specs = (split_slots, P(("lat", "lon"), None, None))
    return jax.shard_map(local, mesh=mesh, in_specs=in_specs, out_specs=out_specs, check_vma=False)
```

```python
import functools

import jax
import jax.numpy as jnp
from jax import lax
from jax.experimental import pallas as pl
from jax.experimental.pallas import tpu as pltpu
from jax.sharding import PartitionSpec as P

MESH = pl.DeviceIdType.MESH
LON = 1280
HALF = LON // 2
TWO_PI = 6.283185307179586
SLOTS = 5
DEVS = 128
ROWS = 5
MEMBERS = 50
WIDTH = 640
SCALES = 3
TILES = WIDTH // 128
GROUPS = ((0, 1), (1, 1), (2, 1), (3, 1), (4, 1))
F32 = jnp.float32
BF16 = jnp.bfloat16


def offsets():
    out = []
    for dx in range(4):
        for dy in range(4):
            for dz in range(4):
                for dc in range(2):
                    if dx or dy or dz or dc:
                        hops = sum(min(d, 4 - d) for d in (dx, dy, dz))
                        out.append((-hops, dx, dy, dz, dc))
    return [o[1:] for o in sorted(out)]


def split(x):
    hi = x.astype(BF16)
    return hi, (x - hi.astype(F32)).astype(BF16)


def dot(a, b, dims=(((1,), (0,)), ((), ()))):
    return lax.dot_general(a, b, dims, preferred_element_type=F32)


def unit(turns):
    near = jnp.round(turns * (1.0 / LON))
    x = (turns - near * LON) * (TWO_PI / LON)
    y = x * x
    c, s = None, None
    for n in range(8, -1, -1):
        a = (-1.0) ** n
        fact = 1.0
        for i in range(1, 2 * n + 1):
            fact *= i
        c = a / fact if c is None else c * y + a / fact
        s = a / (fact * (2 * n + 1)) if s is None else s * y + a / (fact * (2 * n + 1))
    return c, s * x


def exchange_kernel(
    order_hbm, waves_hbm, decay_hbm, amp_hbm, old_hbm, noise_hbm, leg_hbm,
    new_ref, acc_ref, last_ref, sign_ref, last_hi, last_lo,
    order_ref, waves_ref, wave_ref, decay_ref, amp_ref,
    old, noise, leg, total, coef, perm, send, recv, tab_hi, tab_lo,
    small_sem, load_sem, leg_sem, send_sem, recv_sem,
):
    lat = lax.axis_index("lat")
    z = lax.axis_index("lon")
    me = lat * 4 + z
    x, y, c = lat // 8, lax.rem(lat // 2, 4), lax.rem(lat, 2)

    def peer(o):
        dx, dy, dz, dc = o
        px, py, pz = lax.rem(x + dx, 4), lax.rem(y + dy, 4), lax.rem(z + dz, 4)
        pc = lax.rem(c + dc, 2)
        return (px * 4 + py) * 2 + pc, pz

    def load(s):
        for t in range(TILES):
            lanes_of = pl.ds(t * 128, 128)
            pltpu.make_async_copy(old_hbm.at[s, :, :, :, lanes_of], old.at[s, t], load_sem.at[0, s]).start()
            pltpu.make_async_copy(noise_hbm.at[s, :, :, :, lanes_of], noise.at[s, t], load_sem.at[1, s]).start()
        pltpu.make_async_copy(leg_hbm.at[s], leg.at[s], leg_sem.at[s]).start()

    small = [
        pltpu.make_async_copy(src, dst, small_sem.at[i])
        for i, (src, dst) in enumerate(
            [
                (order_hbm, order_ref),
                (waves_hbm, waves_ref),
                (waves_hbm, wave_ref),
                (decay_hbm, decay_ref),
                (amp_hbm, amp_ref),
            ]
        )
    ]
    for copy in small:
        copy.start()
    load(0)
    barrier = pltpu.get_barrier_semaphore()
    peers = [peer(o) for o in offsets()]
    for p in peers:
        pl.semaphore_signal(barrier, inc=1, device_id=p, device_id_type=MESH)
    load(1)
    for copy in small:
        copy.wait()

    at_lane = lax.broadcasted_iota(jnp.int32, (8, WIDTH), 1)
    at_row = lax.broadcasted_iota(jnp.int32, (8, WIDTH), 0)
    kept = at_lane - ((at_lane * 205) >> 10) * ROWS == at_row
    parts = []
    for ref in (order_ref, waves_ref):
        value = jnp.where(kept, ref[...].reshape(1, WIDTH).astype(F32), 0.0)
        parts += list(split(value))
    owner = (lax.broadcasted_iota(jnp.int32, (WIDTH, DEVS), 0) * 205) >> 10
    owner = jnp.where(owner == lax.broadcasted_iota(jnp.int32, (WIDTH, DEVS), 1), 1.0, 0.0).astype(BF16)
    picked = jnp.concatenate([p.astype(F32) for p in parts], axis=0).astype(BF16)
    picked = dot(picked, owner)
    order_rows = picked[0:8] + picked[8:16]
    wave_rows = picked[16:24] + picked[24:32]

    spot = lax.broadcasted_iota(jnp.int32, (DEVS, 128), 1).astype(F32)
    for q in range(ROWS):
        shown = jnp.broadcast_to(order_rows[q : q + 1], (DEVS, 128)).T
        for t in range(TILES):
            hit = jnp.where(spot == shown - 128.0 * t, 1.0, 0.0).astype(BF16)
            perm[q * DEVS : (q + 1) * DEVS, t * 128 : (t + 1) * 128] = hit

    lanes = lax.broadcasted_iota(jnp.int32, (DEVS, 128), 1)
    nt = (((1,), (1,)), ((), ()))
    amp = amp_ref[...]
    coef[...] = jnp.zeros_like(coef)

    def advance(s):
        pltpu.make_async_copy(old.at[s], old.at[s], load_sem.at[0, s]).wait()
        pltpu.make_async_copy(noise.at[s], noise.at[s], load_sem.at[1, s]).wait()
        wave = wave_ref[me * SLOTS + s]
        live = at_lane[0:1] < WIDTH - wave
        shifted = pltpu.roll(amp, lax.rem(WIDTH - wave, WIDTH), 1)
        keep, gain = [], []
        for k in range(SCALES):
            d = jnp.full((1, WIDTH), decay_ref[k], F32)
            keep.append(jnp.where(live, d, 0.0))
            gain.append(jnp.where(live, shifted[k : k + 1] * jnp.sqrt(1.0 - d * d), 0.0))
        for t in range(TILES):
            at = slice(t * 128, (t + 1) * 128)
            summed = None
            for k in range(SCALES):
                fresh = (
                    keep[k][:, at] * old.at[s, t, k].reshape(2 * MEMBERS, 128)[...]
                    + gain[k][:, at] * noise.at[s, t, k].reshape(2 * MEMBERS, 128)[...].astype(F32)
                )
                new_ref.at[s, t, k].reshape(2 * MEMBERS, 128)[...] = fresh
                summed = fresh if summed is None else summed + fresh
            total[t, 0 : 2 * MEMBERS, :] = summed
            for r in range(2):
                coef[r * 64 : r * 64 + MEMBERS, at] = total[t, pl.ds(r, MEMBERS, stride=2), :]

    def field(s):
        advance(s)
        pltpu.make_async_copy(leg_hbm.at[s], leg.at[s], leg_sem.at[s]).wait()
        if s + 2 < SLOTS:
            load(s + 2)
        c_hi, c_lo = split(coef[...])
        l_hi, l_lo = split(leg[s])
        left = jnp.concatenate([l_hi, l_lo], axis=1)
        right = jnp.concatenate(
            [jnp.concatenate([c_hi, c_hi], axis=1), jnp.concatenate([c_lo, jnp.zeros_like(c_lo)], axis=1)], axis=0
        )
        f = dot(left, right, nt)
        f = f[:, 0:128] + f[:, 128:]
        f_hi, f_lo = split(f)
        g = dot(perm[...], jnp.concatenate([f_hi, f_lo], axis=1))
        g = g[:, 0:128] + g[:, 128:]
        for r in range(2):
            low, high = None, None
            for q in range(ROWS):
                block = g[q * DEVS : (q + 1) * DEVS]
                shift = (q * MEMBERS - r * 64) % 128
                if shift:
                    block = pltpu.roll(block, shift, 1)
                start = q * MEMBERS
                if start < 128:
                    low = block if low is None else jnp.where(lanes >= start, block, low)
                if start + MEMBERS > 128:
                    high = block if high is None else jnp.where(lanes >= start - 128, block, high)
            send[s, :, 2 * r, :] = low
            send[s, :, 2 * r + 1, :] = high

    def start(g):
        first, count = GROUPS[g]
        mine = pl.ds(first, count)
        for p in peers:
            pltpu.make_async_remote_copy(
                src_ref=send.at[mine, p[0] * 4 + p[1]],
                dst_ref=recv.at[mine, me],
                send_sem=send_sem.at[g],
                recv_sem=recv_sem.at[g],
                device_id=p,
                device_id_type=MESH,
            ).start()
        for s in range(first, first + count):
            recv[s, pl.ds(me, 1)] = send[s, pl.ds(me, 1)]

    for g, (first, count) in enumerate(GROUPS):
        for s in range(first, first + count):
            field(s)
        if g == 0:
            pl.semaphore_wait(barrier, DEVS - 1)
        start(g)

    turn = [unit(wave_rows * float(n)) for n in (8, 16, 32, 64, 128)]
    small_t = lax.broadcasted_iota(jnp.int32, (8, 128), 0).astype(F32)
    signs = []
    for s in range(SLOTS):
        if s < SLOTS - 1:
            t_hi, t_lo = tab_hi.at[s], tab_lo.at[s]
        else:
            t_hi, t_lo = last_hi, last_lo
        m = wave_rows[s : s + 1]
        weight = jnp.where(m == 0.0, 1.0, 2.0)
        cos, sin = unit(jnp.broadcast_to(m, (8, 128)) * small_t)
        cos, sin = weight * cos, -weight * sin
        for c8, s8 in turn[:4]:
            c8, s8 = c8[s : s + 1], s8[s : s + 1]
            cos, sin = (
                jnp.concatenate([cos, cos * c8 + sin * s8], axis=0),
                jnp.concatenate([sin, sin * c8 - cos * s8], axis=0),
            )
        cos, sin = cos.T, sin.T
        step_c = jnp.broadcast_to(turn[4][0][s : s + 1], (DEVS, 128)).T
        step_s = jnp.broadcast_to(turn[4][1][s : s + 1], (DEVS, 128)).T
        for a in range(TILES):
            at = slice(a * 128, (a + 1) * 128)
            t_hi[0:DEVS, at], t_lo[0:DEVS, at] = split(cos)
            t_hi[DEVS:, at], t_lo[DEVS:, at] = split(sin)
            if a + 1 < TILES:
                cos, sin = cos * step_c + sin * step_s, sin * step_c - cos * step_s
        odd = m - 2.0 * jnp.floor(m * 0.5)
        sign = jnp.broadcast_to(1.0 - 2.0 * odd, (8, 128))
        signs.append(jnp.concatenate([sign, sign], axis=1))
    sign_ref[...] = signs[SLOTS - 1]

    for s in range(SLOTS):
        for g, (first, count) in enumerate(GROUPS):
            if s == first:
                whole = recv.at[pl.ds(first, count), pl.ds(0, DEVS - 1)]
                pltpu.make_async_copy(whole, whole, recv_sem.at[g]).wait()
        rows = []
        for lt in range(2):
            got = jnp.concatenate([recv[s, :, 2 * r + lt, :] for r in range(2)], axis=0)
            rows.append(got.T)
        w = jnp.concatenate(rows, axis=0)
        if s == SLOTS - 1:
            last_ref[...] = w
        elif s == 0:
            acc_ref[...] = synthesize(w, signs[s], tab_hi[s], tab_lo[s])
        else:
            acc_ref[...] += synthesize(w, signs[s], tab_hi[s], tab_lo[s])
    for g, (first, count) in enumerate(GROUPS):
        whole = send.at[pl.ds(first, count), pl.ds(0, DEVS - 1)]
        pltpu.make_async_copy(whole, whole, send_sem.at[g]).wait()


def synthesize(w, sign, t_hi, t_lo):
    w_hi, w_lo = split(w)
    sg = sign[0:1].astype(BF16)
    left_hi = jnp.concatenate([w_hi, w_hi * sg], axis=0)
    left_lo = jnp.concatenate([w_lo, w_lo * sg], axis=0)
    return dot(jnp.concatenate([left_hi, left_lo], axis=0), t_hi).reshape(2, 512, HALF).sum(0) + dot(left_hi, t_lo)


def finish_kernel(new_ref, acc_ref, last_ref, sign_ref, last_hi, last_lo, new_hbm, out_hbm, out, new_sem, out_sem):
    for s in range(SLOTS):
        for t in range(TILES):
            pltpu.make_async_copy(
                new_ref.at[s, t], new_hbm.at[s, :, :, :, pl.ds(t * 128, 128)], new_sem.at[s]
            ).start()
    both = acc_ref[...] + synthesize(last_ref[...], sign_ref[...], last_hi[...], last_lo[...])
    for q in range(ROWS):
        for h in range(2):
            base = h * 256 + q * MEMBERS
            out[q, :, h * HALF : (h + 1) * HALF] = both[base : base + MEMBERS, :]
        pltpu.make_async_copy(out.at[q], out_hbm.at[q], out_sem.at[q]).start()
    for q in range(ROWS):
        pltpu.make_async_copy(out.at[q], out_hbm.at[q], out_sem.at[q]).wait()
    for s in range(SLOTS):
        pltpu.make_async_copy(new_ref.at[s], new_ref.at[s], new_sem.at[s]).wait()


def local(coeffs_old, noise, legendre, decay, amplitude, wavenumber_of_slot, lat_order):
    old = coeffs_old.transpose(0, 2, 3, 1, 4)
    fresh = noise.transpose(0, 2, 3, 1, 4)
    vmem = pl.BlockSpec(memory_space=pltpu.VMEM)
    hbm = pl.BlockSpec(memory_space=pltpu.HBM)
    block = (SLOTS, TILES, SCALES, MEMBERS, 2, 128)
    kept = pl.pallas_call(
        exchange_kernel,
        name="exchange",
        out_shape=(
            pltpu.VMEM(block, F32),
            pltpu.VMEM((512, HALF), F32),
            pltpu.VMEM((256, 256), F32),
            pltpu.VMEM((8, 256), F32),
            pltpu.VMEM((2 * DEVS, HALF), BF16),
            pltpu.VMEM((2 * DEVS, HALF), BF16),
        ),
        in_specs=[hbm] * 7,
        out_specs=(vmem,) * 6,
        scratch_shapes=[
            pltpu.VMEM((WIDTH,), jnp.int32),
            pltpu.VMEM((WIDTH,), jnp.int32),
            pltpu.SMEM((WIDTH,), jnp.int32),
            pltpu.SMEM((SCALES,), F32),
            pltpu.VMEM((SCALES, WIDTH), F32),
            pltpu.VMEM(block, F32),
            pltpu.VMEM(block, BF16),
            pltpu.VMEM((SLOTS, WIDTH, WIDTH), F32),
            pltpu.VMEM((TILES, 104, 128), F32),
            pltpu.VMEM((128, WIDTH), F32),
            pltpu.VMEM((WIDTH, WIDTH), BF16),
            pltpu.VMEM((SLOTS, DEVS, 4, 128), F32),
            pltpu.VMEM((SLOTS, DEVS, 4, 128), F32),
            pltpu.VMEM((SLOTS - 1, 2 * DEVS, HALF), BF16),
            pltpu.VMEM((SLOTS - 1, 2 * DEVS, HALF), BF16),
            pltpu.SemaphoreType.DMA((5,)),
            pltpu.SemaphoreType.DMA((2, SLOTS)),
            pltpu.SemaphoreType.DMA((SLOTS,)),
            pltpu.SemaphoreType.DMA((len(GROUPS),)),
            pltpu.SemaphoreType.DMA((len(GROUPS),)),
        ],
        compiler_params=pltpu.CompilerParams(collective_id=0, has_side_effects=True, vmem_limit_bytes=44 * 2**20),
    )(*(pltpu.with_memory_space_constraint(v, pltpu.HBM) for v in (lat_order, wavenumber_of_slot, decay, amplitude, old, fresh, legendre)))
    new, pattern = pl.pallas_call(
        finish_kernel,
        name="finish",
        out_shape=(
            jax.ShapeDtypeStruct((SLOTS, SCALES, MEMBERS, 2, WIDTH), F32),
            jax.ShapeDtypeStruct((ROWS, MEMBERS, LON), F32),
        ),
        in_specs=[vmem] * 6,
        out_specs=(hbm, hbm),
        scratch_shapes=[
            pltpu.VMEM((ROWS, MEMBERS, LON), F32),
            pltpu.SemaphoreType.DMA((SLOTS,)),
            pltpu.SemaphoreType.DMA((ROWS,)),
        ],
        compiler_params=pltpu.CompilerParams(vmem_limit_bytes=24 * 2**20),
    )(*kept)
    return new.transpose(0, 3, 1, 2, 4), pattern


def solution(mesh):
    split_slots = P(("lat", "lon"), None, None, None, None)
    in_specs = (split_slots, split_slots, P(("lat", "lon"), None, None), P(), P(), P(), P())
    out_specs = (split_slots, P(("lat", "lon"), None, None))
    return jax.shard_map(local, mesh=mesh, in_specs=in_specs, out_specs=out_specs, check_vma=False)
```

```python
import functools

import jax
import jax.numpy as jnp
from jax import lax
from jax.experimental import pallas as pl
from jax.experimental.pallas import tpu as pltpu
from jax.sharding import PartitionSpec as P

MESH = pl.DeviceIdType.MESH
LON = 1280
HALF = LON // 2
TWO_PI = 6.283185307179586
SLOTS = 5
DEVS = 128
ROWS = 5
MEMBERS = 50
WIDTH = 640
SCALES = 3
TILES = WIDTH // 128
GROUPS = ((0, 1), (1, 1), (2, 1), (3, 1), (4, 1))
F32 = jnp.float32
BF16 = jnp.bfloat16


def offsets():
    out = []
    for dx in range(4):
        for dy in range(4):
            for dz in range(4):
                for dc in range(2):
                    if dx or dy or dz or dc:
                        hops = sum(min(d, 4 - d) for d in (dx, dy, dz))
                        out.append((-hops, dx, dy, dz, dc))
    return [o[1:] for o in sorted(out)]


def split(x):
    hi = x.astype(BF16)
    return hi, (x - hi.astype(F32)).astype(BF16)


def dot(a, b, dims=(((1,), (0,)), ((), ()))):
    return lax.dot_general(a, b, dims, preferred_element_type=F32)


def unit(turns):
    near = jnp.round(turns * (1.0 / LON))
    x = (turns - near * LON) * (TWO_PI / LON)
    y = x * x
    c, s = None, None
    for n in range(8, -1, -1):
        a = (-1.0) ** n
        fact = 1.0
        for i in range(1, 2 * n + 1):
            fact *= i
        c = a / fact if c is None else c * y + a / fact
        s = a / (fact * (2 * n + 1)) if s is None else s * y + a / (fact * (2 * n + 1))
    return c, s * x


def exchange_kernel(
    order_hbm, waves_hbm, decay_hbm, amp_hbm, old_hbm, noise_hbm, leg_hbm,
    new_ref, acc_ref, last_ref, sign_ref, last_hi, last_lo,
    order_ref, waves_ref, wave_ref, decay_ref, amp_ref,
    old, noise, leg, total, coef, perm, send, recv, tab_hi, tab_lo,
    small_sem, load_sem, leg_sem, send_sem, recv_sem,
):
    lat = lax.axis_index("lat")
    z = lax.axis_index("lon")
    me = lat * 4 + z
    x, y, c = lat // 8, lax.rem(lat // 2, 4), lax.rem(lat, 2)

    def peer(o):
        dx, dy, dz, dc = o
        px, py, pz = lax.rem(x + dx, 4), lax.rem(y + dy, 4), lax.rem(z + dz, 4)
        pc = lax.rem(c + dc, 2)
        return (px * 4 + py) * 2 + pc, pz

    noise_rows = noise_hbm.reshape(SLOTS, SCALES, 2 * MEMBERS, WIDTH)

    def load(s):
        for t in range(TILES):
            lanes_of = pl.ds(t * 128, 128)
            pltpu.make_async_copy(old_hbm.at[s, :, :, :, lanes_of], old.at[s, t], load_sem.at[0, s]).start()
            pltpu.make_async_copy(
                noise_rows.at[s, :, :, lanes_of], noise.at[s, t, :, 0 : 2 * MEMBERS], load_sem.at[1, s]
            ).start()
        pltpu.make_async_copy(leg_hbm.at[s], leg.at[s], leg_sem.at[s]).start()

    small = [
        pltpu.make_async_copy(src, dst, small_sem.at[i])
        for i, (src, dst) in enumerate(
            [
                (order_hbm, order_ref),
                (waves_hbm, waves_ref),
                (waves_hbm, wave_ref),
                (decay_hbm, decay_ref),
                (amp_hbm, amp_ref),
            ]
        )
    ]
    for copy in small:
        copy.start()
    load(0)
    barrier = pltpu.get_barrier_semaphore()
    peers = [peer(o) for o in offsets()]
    for p in peers:
        pl.semaphore_signal(barrier, inc=1, device_id=p, device_id_type=MESH)
    load(1)
    for copy in small:
        copy.wait()

    at_lane = lax.broadcasted_iota(jnp.int32, (8, WIDTH), 1)
    at_row = lax.broadcasted_iota(jnp.int32, (8, WIDTH), 0)
    kept = at_lane - ((at_lane * 205) >> 10) * ROWS == at_row
    parts = []
    for ref in (order_ref, waves_ref):
        value = jnp.where(kept, ref[...].reshape(1, WIDTH).astype(F32), 0.0)
        parts += list(split(value))
    owner = (lax.broadcasted_iota(jnp.int32, (WIDTH, DEVS), 0) * 205) >> 10
    owner = jnp.where(owner == lax.broadcasted_iota(jnp.int32, (WIDTH, DEVS), 1), 1.0, 0.0).astype(BF16)
    picked = jnp.concatenate([p.astype(F32) for p in parts], axis=0).astype(BF16)
    picked = dot(picked, owner)
    order_rows = picked[0:8] + picked[8:16]
    wave_rows = picked[16:24] + picked[24:32]

    spot = lax.broadcasted_iota(jnp.int32, (DEVS, 128), 1).astype(F32)
    for q in range(ROWS):
        shown = jnp.broadcast_to(order_rows[q : q + 1], (DEVS, 128)).T
        for t in range(TILES):
            hit = jnp.where(spot == shown - 128.0 * t, 1.0, 0.0).astype(BF16)
            perm[q * DEVS : (q + 1) * DEVS, t * 128 : (t + 1) * 128] = hit

    lanes = lax.broadcasted_iota(jnp.int32, (DEVS, 128), 1)
    nt = (((1,), (1,)), ((), ()))
    amp = amp_ref[...]
    coef[...] = jnp.zeros_like(coef)

    def advance(s):
        pltpu.make_async_copy(old.at[s], old.at[s], load_sem.at[0, s]).wait()
        whole = noise.at[s, :, :, 0 : 2 * MEMBERS]
        pltpu.make_async_copy(whole, whole, load_sem.at[1, s]).wait()
        wave = wave_ref[me * SLOTS + s]
        live = at_lane[0:1] < WIDTH - wave
        shifted = pltpu.roll(amp, lax.rem(WIDTH - wave, WIDTH), 1)
        keep, gain = [], []
        for k in range(SCALES):
            d = jnp.full((1, WIDTH), decay_ref[k], F32)
            keep.append(jnp.where(live, d, 0.0))
            gain.append(jnp.where(live, shifted[k : k + 1] * jnp.sqrt(1.0 - d * d), 0.0))
        for t in range(TILES):
            at = slice(t * 128, (t + 1) * 128)
            summed = None
            for k in range(SCALES):
                fresh = (
                    keep[k][:, at] * old.at[s, t, k].reshape(2 * MEMBERS, 128)[...]
                    + gain[k][:, at] * noise[s, t, k, 0 : 2 * MEMBERS, :].astype(F32)
                )
                new_ref.at[s, t, k].reshape(2 * MEMBERS, 128)[...] = fresh
                summed = fresh if summed is None else summed + fresh
            total[t, 0 : 2 * MEMBERS, :] = summed
            for r in range(2):
                coef[r * 64 : r * 64 + MEMBERS, at] = total[t, pl.ds(r, MEMBERS, stride=2), :]

    def field(s):
        advance(s)
        pltpu.make_async_copy(leg_hbm.at[s], leg.at[s], leg_sem.at[s]).wait()
        if s + 2 < SLOTS:
            load(s + 2)
        c_hi, c_lo = split(coef[...])
        l_hi, l_lo = split(leg[s])
        left = jnp.concatenate([l_hi, l_lo], axis=1)
        right = jnp.concatenate(
            [jnp.concatenate([c_hi, c_hi], axis=1), jnp.concatenate([c_lo, jnp.zeros_like(c_lo)], axis=1)], axis=0
        )
        f = dot(left, right, nt)
        f = f[:, 0:128] + f[:, 128:]
        f_hi, f_lo = split(f)
        g = dot(perm[...], jnp.concatenate([f_hi, f_lo], axis=1))
        g = g[:, 0:128] + g[:, 128:]
        for r in range(2):
            low, high = None, None
            for q in range(ROWS):
                block = g[q * DEVS : (q + 1) * DEVS]
                shift = (q * MEMBERS - r * 64) % 128
                if shift:
                    block = pltpu.roll(block, shift, 1)
                start = q * MEMBERS
                if start < 128:
                    low = block if low is None else jnp.where(lanes >= start, block, low)
                if start + MEMBERS > 128:
                    high = block if high is None else jnp.where(lanes >= start - 128, block, high)
            send[s, :, 2 * r, :] = low
            send[s, :, 2 * r + 1, :] = high

    def start(g):
        first, count = GROUPS[g]
        mine = pl.ds(first, count)
        for p in peers:
            pltpu.make_async_remote_copy(
                src_ref=send.at[mine, p[0] * 4 + p[1]],
                dst_ref=recv.at[mine, me],
                send_sem=send_sem.at[g],
                recv_sem=recv_sem.at[g],
                device_id=p,
                device_id_type=MESH,
            ).start()
        for s in range(first, first + count):
            recv[s, pl.ds(me, 1)] = send[s, pl.ds(me, 1)]

    for g, (first, count) in enumerate(GROUPS):
        for s in range(first, first + count):
            field(s)
        if g == 0:
            pl.semaphore_wait(barrier, DEVS - 1)
        start(g)

    turn = [unit(wave_rows * float(n)) for n in (8, 16, 32, 64, 128)]
    small_t = lax.broadcasted_iota(jnp.int32, (8, 128), 0).astype(F32)
    signs = []
    for s in range(SLOTS):
        if s < SLOTS - 1:
            t_hi, t_lo = tab_hi.at[s], tab_lo.at[s]
        else:
            t_hi, t_lo = last_hi, last_lo
        m = wave_rows[s : s + 1]
        weight = jnp.where(m == 0.0, 1.0, 2.0)
        cos, sin = unit(jnp.broadcast_to(m, (8, 128)) * small_t)
        cos, sin = weight * cos, -weight * sin
        for c8, s8 in turn[:4]:
            c8, s8 = c8[s : s + 1], s8[s : s + 1]
            cos, sin = (
                jnp.concatenate([cos, cos * c8 + sin * s8], axis=0),
                jnp.concatenate([sin, sin * c8 - cos * s8], axis=0),
            )
        cos, sin = cos.T, sin.T
        step_c = jnp.broadcast_to(turn[4][0][s : s + 1], (DEVS, 128)).T
        step_s = jnp.broadcast_to(turn[4][1][s : s + 1], (DEVS, 128)).T
        for a in range(TILES):
            at = slice(a * 128, (a + 1) * 128)
            t_hi[0:DEVS, at], t_lo[0:DEVS, at] = split(cos)
            t_hi[DEVS:, at], t_lo[DEVS:, at] = split(sin)
            if a + 1 < TILES:
                cos, sin = cos * step_c + sin * step_s, sin * step_c - cos * step_s
        odd = m - 2.0 * jnp.floor(m * 0.5)
        sign = jnp.broadcast_to(1.0 - 2.0 * odd, (8, 128))
        signs.append(jnp.concatenate([sign, sign], axis=1))
    sign_ref[...] = signs[SLOTS - 1]

    for s in range(SLOTS):
        for g, (first, count) in enumerate(GROUPS):
            if s == first:
                whole = recv.at[pl.ds(first, count), pl.ds(0, DEVS - 1)]
                pltpu.make_async_copy(whole, whole, recv_sem.at[g]).wait()
        rows = []
        for lt in range(2):
            got = jnp.concatenate([recv[s, :, 2 * r + lt, :] for r in range(2)], axis=0)
            rows.append(got.T)
        w = jnp.concatenate(rows, axis=0)
        if s == SLOTS - 1:
            last_ref[...] = w
        elif s == 0:
            acc_ref[...] = synthesize(w, signs[s], tab_hi[s], tab_lo[s])
        else:
            acc_ref[...] += synthesize(w, signs[s], tab_hi[s], tab_lo[s])
    for g, (first, count) in enumerate(GROUPS):
        whole = send.at[pl.ds(first, count), pl.ds(0, DEVS - 1)]
        pltpu.make_async_copy(whole, whole, send_sem.at[g]).wait()


def synthesize(w, sign, t_hi, t_lo):
    w_hi, w_lo = split(w)
    sg = sign[0:1].astype(BF16)
    left_hi = jnp.concatenate([w_hi, w_hi * sg], axis=0)
    left_lo = jnp.concatenate([w_lo, w_lo * sg], axis=0)
    return dot(jnp.concatenate([left_hi, left_lo], axis=0), t_hi).reshape(2, 512, HALF).sum(0) + dot(left_hi, t_lo)


def finish_kernel(new_ref, acc_ref, last_ref, sign_ref, last_hi, last_lo, new_hbm, out_hbm, out, new_sem, out_sem):
    for s in range(SLOTS):
        for t in range(TILES):
            pltpu.make_async_copy(
                new_ref.at[s, t], new_hbm.at[s, :, :, :, pl.ds(t * 128, 128)], new_sem.at[s]
            ).start()
    both = acc_ref[...] + synthesize(last_ref[...], sign_ref[...], last_hi[...], last_lo[...])
    for q in range(ROWS):
        for h in range(2):
            base = h * 256 + q * MEMBERS
            out[q, :, h * HALF : (h + 1) * HALF] = both[base : base + MEMBERS, :]
        pltpu.make_async_copy(out.at[q], out_hbm.at[q], out_sem.at[q]).start()
    for q in range(ROWS):
        pltpu.make_async_copy(out.at[q], out_hbm.at[q], out_sem.at[q]).wait()
    for s in range(SLOTS):
        pltpu.make_async_copy(new_ref.at[s], new_ref.at[s], new_sem.at[s]).wait()


def local(coeffs_old, noise, legendre, decay, amplitude, wavenumber_of_slot, lat_order):
    old = coeffs_old.transpose(0, 2, 3, 1, 4)
    fresh = noise.transpose(0, 2, 3, 1, 4)
    vmem = pl.BlockSpec(memory_space=pltpu.VMEM)
    hbm = pl.BlockSpec(memory_space=pltpu.HBM)
    block = (SLOTS, TILES, SCALES, MEMBERS, 2, 128)
    kept = pl.pallas_call(
        exchange_kernel,
        name="exchange",
        out_shape=(
            pltpu.VMEM(block, F32),
            pltpu.VMEM((512, HALF), F32),
            pltpu.VMEM((256, 256), F32),
            pltpu.VMEM((8, 256), F32),
            pltpu.VMEM((2 * DEVS, HALF), BF16),
            pltpu.VMEM((2 * DEVS, HALF), BF16),
        ),
        in_specs=[hbm] * 7,
        out_specs=(vmem,) * 6,
        scratch_shapes=[
            pltpu.VMEM((WIDTH,), jnp.int32),
            pltpu.VMEM((WIDTH,), jnp.int32),
            pltpu.SMEM((WIDTH,), jnp.int32),
            pltpu.SMEM((SCALES,), F32),
            pltpu.VMEM((SCALES, WIDTH), F32),
            pltpu.VMEM(block, F32),
            pltpu.VMEM((SLOTS, TILES, SCALES, 112, 128), BF16),
            pltpu.VMEM((SLOTS, WIDTH, WIDTH), F32),
            pltpu.VMEM((TILES, 104, 128), F32),
            pltpu.VMEM((128, WIDTH), F32),
            pltpu.VMEM((WIDTH, WIDTH), BF16),
            pltpu.VMEM((SLOTS, DEVS, 4, 128), F32),
            pltpu.VMEM((SLOTS, DEVS, 4, 128), F32),
            pltpu.VMEM((SLOTS - 1, 2 * DEVS, HALF), BF16),
            pltpu.VMEM((SLOTS - 1, 2 * DEVS, HALF), BF16),
            pltpu.SemaphoreType.DMA((5,)),
            pltpu.SemaphoreType.DMA((2, SLOTS)),
            pltpu.SemaphoreType.DMA((SLOTS,)),
            pltpu.SemaphoreType.DMA((len(GROUPS),)),
            pltpu.SemaphoreType.DMA((len(GROUPS),)),
        ],
        compiler_params=pltpu.CompilerParams(collective_id=0, has_side_effects=True, vmem_limit_bytes=44 * 2**20),
    )(*(pltpu.with_memory_space_constraint(v, pltpu.HBM) for v in (lat_order, wavenumber_of_slot, decay, amplitude, old, fresh, legendre)))
    new, pattern = pl.pallas_call(
        finish_kernel,
        name="finish",
        out_shape=(
            jax.ShapeDtypeStruct((SLOTS, SCALES, MEMBERS, 2, WIDTH), F32),
            jax.ShapeDtypeStruct((ROWS, MEMBERS, LON), F32),
        ),
        in_specs=[vmem] * 6,
        out_specs=(hbm, hbm),
        scratch_shapes=[
            pltpu.VMEM((ROWS, MEMBERS, LON), F32),
            pltpu.SemaphoreType.DMA((SLOTS,)),
            pltpu.SemaphoreType.DMA((ROWS,)),
        ],
        compiler_params=pltpu.CompilerParams(vmem_limit_bytes=24 * 2**20),
    )(*kept)
    return new.transpose(0, 3, 1, 2, 4), pattern


def solution(mesh):
    split_slots = P(("lat", "lon"), None, None, None, None)
    in_specs = (split_slots, split_slots, P(("lat", "lon"), None, None), P(), P(), P(), P())
    out_specs = (split_slots, P(("lat", "lon"), None, None))
    return jax.shard_map(local, mesh=mesh, in_specs=in_specs, out_specs=out_specs, check_vma=False)
```

```python
import functools

import jax
import jax.numpy as jnp
from jax import lax
from jax.experimental import pallas as pl
from jax.experimental.pallas import tpu as pltpu
from jax.sharding import PartitionSpec as P

MESH = pl.DeviceIdType.MESH
LON = 1280
HALF = LON // 2
TWO_PI = 6.283185307179586
SLOTS = 5
DEVS = 128
ROWS = 5
MEMBERS = 50
WIDTH = 640
SCALES = 3
TILES = WIDTH // 128
GROUPS = ((0, 1), (1, 1), (2, 1), (3, 1), (4, 1))
F32 = jnp.float32
BF16 = jnp.bfloat16


def offsets():
    out = []
    for dx in range(4):
        for dy in range(4):
            for dz in range(4):
                for dc in range(2):
                    if dx or dy or dz or dc:
                        hops = sum(min(d, 4 - d) for d in (dx, dy, dz))
                        out.append((-hops, dx, dy, dz, dc))
    return [o[1:] for o in sorted(out)]


def split(x):
    hi = x.astype(BF16)
    return hi, (x - hi.astype(F32)).astype(BF16)


def dot(a, b, dims=(((1,), (0,)), ((), ()))):
    return lax.dot_general(a, b, dims, preferred_element_type=F32)


def unit(turns):
    near = jnp.round(turns * (1.0 / LON))
    x = (turns - near * LON) * (TWO_PI / LON)
    y = x * x
    c, s = None, None
    for n in range(8, -1, -1):
        a = (-1.0) ** n
        fact = 1.0
        for i in range(1, 2 * n + 1):
            fact *= i
        c = a / fact if c is None else c * y + a / fact
        s = a / (fact * (2 * n + 1)) if s is None else s * y + a / (fact * (2 * n + 1))
    return c, s * x


def exchange_kernel(
    order_hbm, waves_hbm, decay_hbm, amp_hbm, old_hbm, noise_hbm, leg_hbm,
    new_ref, acc_ref, last_ref, sign_ref, last_hi, last_lo,
    order_ref, waves_ref, wave_ref, decay_ref, amp_ref,
    old, noise, leg, total, coef, perm, send, recv, tab_hi, tab_lo,
    small_sem, load_sem, leg_sem, send_sem, recv_sem,
):
    lat = lax.axis_index("lat")
    z = lax.axis_index("lon")
    me = lat * 4 + z
    x, y, c = lat // 8, lax.rem(lat // 2, 4), lax.rem(lat, 2)

    def peer(o):
        dx, dy, dz, dc = o
        px, py, pz = lax.rem(x + dx, 4), lax.rem(y + dy, 4), lax.rem(z + dz, 4)
        pc = lax.rem(c + dc, 2)
        return (px * 4 + py) * 2 + pc, pz

    noise_rows = noise_hbm.reshape(SLOTS, SCALES, 2 * MEMBERS, WIDTH)

    def load(s):
        for t in range(TILES):
            lanes_of = pl.ds(t * 128, 128)
            pltpu.make_async_copy(old_hbm.at[s, :, :, :, lanes_of], old.at[s, t], load_sem.at[0, s]).start()
            pltpu.make_async_copy(
                noise_rows.at[s, :, :, lanes_of], noise.at[s, t, :, 0 : 2 * MEMBERS], load_sem.at[1, s]
            ).start()
        pltpu.make_async_copy(leg_hbm.at[s], leg.at[s], leg_sem.at[s]).start()

    small = [
        pltpu.make_async_copy(src, dst, small_sem.at[i])
        for i, (src, dst) in enumerate(
            [
                (order_hbm, order_ref),
                (waves_hbm, waves_ref),
                (waves_hbm, wave_ref),
                (decay_hbm, decay_ref),
                (amp_hbm, amp_ref),
            ]
        )
    ]
    for copy in small:
        copy.start()
    load(0)
    barrier = pltpu.get_barrier_semaphore()
    peers = [peer(o) for o in offsets()]
    for p in peers:
        pl.semaphore_signal(barrier, inc=1, device_id=p, device_id_type=MESH)
    load(1)
    for copy in small:
        copy.wait()

    at_lane = lax.broadcasted_iota(jnp.int32, (8, WIDTH), 1)
    at_row = lax.broadcasted_iota(jnp.int32, (8, WIDTH), 0)
    kept = at_lane - ((at_lane * 205) >> 10) * ROWS == at_row
    parts = []
    for ref in (order_ref, waves_ref):
        value = jnp.where(kept, ref[...].reshape(1, WIDTH).astype(F32), 0.0)
        parts += list(split(value))
    owner = (lax.broadcasted_iota(jnp.int32, (WIDTH, DEVS), 0) * 205) >> 10
    owner = jnp.where(owner == lax.broadcasted_iota(jnp.int32, (WIDTH, DEVS), 1), 1.0, 0.0).astype(BF16)
    picked = jnp.concatenate([p.astype(F32) for p in parts], axis=0).astype(BF16)
    picked = dot(picked, owner)
    order_rows = picked[0:8] + picked[8:16]
    wave_rows = picked[16:24] + picked[24:32]

    spot = lax.broadcasted_iota(jnp.int32, (DEVS, 128), 1).astype(F32)
    for q in range(ROWS):
        shown = jnp.broadcast_to(order_rows[q : q + 1], (DEVS, 128)).T
        for t in range(TILES):
            hit = jnp.where(spot == shown - 128.0 * t, 1.0, 0.0).astype(BF16)
            perm[q * DEVS : (q + 1) * DEVS, t * 128 : (t + 1) * 128] = hit

    lanes = lax.broadcasted_iota(jnp.int32, (DEVS, 128), 1)
    nt = (((1,), (1,)), ((), ()))
    amp = amp_ref[...]
    coef[...] = jnp.zeros_like(coef)

    def advance(s):
        pltpu.make_async_copy(old.at[s], old.at[s], load_sem.at[0, s]).wait()
        whole = noise.at[s, :, :, 0 : 2 * MEMBERS]
        pltpu.make_async_copy(whole, whole, load_sem.at[1, s]).wait()
        wave = wave_ref[me * SLOTS + s]
        live = at_lane[0:1] < WIDTH - wave
        shifted = pltpu.roll(amp, lax.rem(WIDTH - wave, WIDTH), 1)
        keep, gain = [], []
        for k in range(SCALES):
            d = jnp.full((1, WIDTH), decay_ref[k], F32)
            keep.append(jnp.where(live, d, 0.0))
            gain.append(jnp.where(live, shifted[k : k + 1] * jnp.sqrt(1.0 - d * d), 0.0))
        for t in range(TILES):
            at = slice(t * 128, (t + 1) * 128)
            summed = None
            for k in range(SCALES):
                fresh = (
                    keep[k][:, at] * old.at[s, t, k].reshape(2 * MEMBERS, 128)[...]
                    + gain[k][:, at] * noise[s, t, k, 0 : 2 * MEMBERS, :].astype(F32)
                )
                new_ref.at[s, t, k].reshape(2 * MEMBERS, 128)[...] = fresh
                summed = fresh if summed is None else summed + fresh
            total[t, 0 : 2 * MEMBERS, :] = summed
            for r in range(2):
                coef[r * 64 : r * 64 + MEMBERS, at] = total[t, pl.ds(r, MEMBERS, stride=2), :]

    def field(s):
        advance(s)
        pltpu.make_async_copy(leg_hbm.at[s], leg.at[s], leg_sem.at[s]).wait()
        if s + 2 < SLOTS:
            load(s + 2)
        c_hi, c_lo = split(coef[...])
        l_hi, l_lo = split(leg[s])
        f = dot(l_hi, jnp.concatenate([c_hi, c_lo], axis=0), nt)
        f = f[:, 0:128] + (f[:, 128:] + dot(l_lo, c_hi, nt))
        f_hi, f_lo = split(f)
        g = dot(perm[...], jnp.concatenate([f_hi, f_lo], axis=1))
        g = g[:, 0:128] + g[:, 128:]
        for r in range(2):
            low, high = None, None
            for q in range(ROWS):
                block = g[q * DEVS : (q + 1) * DEVS]
                shift = (q * MEMBERS - r * 64) % 128
                if shift:
                    block = pltpu.roll(block, shift, 1)
                start = q * MEMBERS
                if start < 128:
                    low = block if low is None else jnp.where(lanes >= start, block, low)
                if start + MEMBERS > 128:
                    high = block if high is None else jnp.where(lanes >= start - 128, block, high)
            send[s, :, 2 * r, :] = low
            send[s, :, 2 * r + 1, :] = high

    def start(g):
        first, count = GROUPS[g]
        mine = pl.ds(first, count)
        for p in peers:
            pltpu.make_async_remote_copy(
                src_ref=send.at[mine, p[0] * 4 + p[1]],
                dst_ref=recv.at[mine, me],
                send_sem=send_sem.at[g],
                recv_sem=recv_sem.at[g],
                device_id=p,
                device_id_type=MESH,
            ).start()
        for s in range(first, first + count):
            recv[s, pl.ds(me, 1)] = send[s, pl.ds(me, 1)]

    for g, (first, count) in enumerate(GROUPS):
        for s in range(first, first + count):
            field(s)
        if g == 0:
            pl.semaphore_wait(barrier, DEVS - 1)
        start(g)

    turn = [unit(wave_rows * float(n)) for n in (8, 16, 32, 64, 128)]
    small_t = lax.broadcasted_iota(jnp.int32, (8, 128), 0).astype(F32)
    signs = []
    for s in range(SLOTS):
        if s < SLOTS - 1:
            t_hi, t_lo = tab_hi.at[s], tab_lo.at[s]
        else:
            t_hi, t_lo = last_hi, last_lo
        m = wave_rows[s : s + 1]
        weight = jnp.where(m == 0.0, 1.0, 2.0)
        cos, sin = unit(jnp.broadcast_to(m, (8, 128)) * small_t)
        cos, sin = weight * cos, -weight * sin
        for c8, s8 in turn[:4]:
            c8, s8 = c8[s : s + 1], s8[s : s + 1]
            cos, sin = (
                jnp.concatenate([cos, cos * c8 + sin * s8], axis=0),
                jnp.concatenate([sin, sin * c8 - cos * s8], axis=0),
            )
        cos, sin = cos.T, sin.T
        step_c = jnp.broadcast_to(turn[4][0][s : s + 1], (DEVS, 128)).T
        step_s = jnp.broadcast_to(turn[4][1][s : s + 1], (DEVS, 128)).T
        for a in range(TILES):
            at = slice(a * 128, (a + 1) * 128)
            t_hi[0:DEVS, at], t_lo[0:DEVS, at] = split(cos)
            t_hi[DEVS:, at], t_lo[DEVS:, at] = split(sin)
            if a + 1 < TILES:
                cos, sin = cos * step_c + sin * step_s, sin * step_c - cos * step_s
        odd = m - 2.0 * jnp.floor(m * 0.5)
        sign = jnp.broadcast_to(1.0 - 2.0 * odd, (8, 128))
        signs.append(jnp.concatenate([sign, sign], axis=1))
    sign_ref[...] = signs[SLOTS - 1]

    for s in range(SLOTS):
        for g, (first, count) in enumerate(GROUPS):
            if s == first:
                whole = recv.at[pl.ds(first, count), pl.ds(0, DEVS - 1)]
                pltpu.make_async_copy(whole, whole, recv_sem.at[g]).wait()
        rows = []
        for lt in range(2):
            got = jnp.concatenate([recv[s, :, 2 * r + lt, :] for r in range(2)], axis=0)
            rows.append(got.T)
        w = jnp.concatenate(rows, axis=0)
        if s == SLOTS - 1:
            last_ref[...] = w
        elif s == 0:
            acc_ref[...] = synthesize(w, signs[s], tab_hi[s], tab_lo[s])
        else:
            acc_ref[...] += synthesize(w, signs[s], tab_hi[s], tab_lo[s])
    for g, (first, count) in enumerate(GROUPS):
        whole = send.at[pl.ds(first, count), pl.ds(0, DEVS - 1)]
        pltpu.make_async_copy(whole, whole, send_sem.at[g]).wait()


def synthesize(w, sign, t_hi, t_lo):
    w_hi, w_lo = split(w)
    sg = sign[0:1].astype(BF16)
    left_hi = jnp.concatenate([w_hi, w_hi * sg], axis=0)
    left_lo = jnp.concatenate([w_lo, w_lo * sg], axis=0)
    return dot(jnp.concatenate([left_hi, left_lo], axis=0), t_hi).reshape(2, 512, HALF).sum(0) + dot(left_hi, t_lo)


def finish_kernel(new_ref, acc_ref, last_ref, sign_ref, last_hi, last_lo, new_hbm, out_hbm, out, new_sem, out_sem):
    for s in range(SLOTS):
        for t in range(TILES):
            pltpu.make_async_copy(
                new_ref.at[s, t], new_hbm.at[s, :, :, :, pl.ds(t * 128, 128)], new_sem.at[s]
            ).start()
    both = acc_ref[...] + synthesize(last_ref[...], sign_ref[...], last_hi[...], last_lo[...])
    for q in range(ROWS):
        for h in range(2):
            base = h * 256 + q * MEMBERS
            out[q, :, h * HALF : (h + 1) * HALF] = both[base : base + MEMBERS, :]
        pltpu.make_async_copy(out.at[q], out_hbm.at[q], out_sem.at[q]).start()
    for q in range(ROWS):
        pltpu.make_async_copy(out.at[q], out_hbm.at[q], out_sem.at[q]).wait()
    for s in range(SLOTS):
        pltpu.make_async_copy(new_ref.at[s], new_ref.at[s], new_sem.at[s]).wait()


def local(coeffs_old, noise, legendre, decay, amplitude, wavenumber_of_slot, lat_order):
    old = coeffs_old.transpose(0, 2, 3, 1, 4)
    fresh = noise.transpose(0, 2, 3, 1, 4)
    vmem = pl.BlockSpec(memory_space=pltpu.VMEM)
    hbm = pl.BlockSpec(memory_space=pltpu.HBM)
    block = (SLOTS, TILES, SCALES, MEMBERS, 2, 128)
    kept = pl.pallas_call(
        exchange_kernel,
        name="exchange",
        out_shape=(
            pltpu.VMEM(block, F32),
            pltpu.VMEM((512, HALF), F32),
            pltpu.VMEM((256, 256), F32),
            pltpu.VMEM((8, 256), F32),
            pltpu.VMEM((2 * DEVS, HALF), BF16),
            pltpu.VMEM((2 * DEVS, HALF), BF16),
        ),
        in_specs=[hbm] * 7,
        out_specs=(vmem,) * 6,
        scratch_shapes=[
            pltpu.VMEM((WIDTH,), jnp.int32),
            pltpu.VMEM((WIDTH,), jnp.int32),
            pltpu.SMEM((WIDTH,), jnp.int32),
            pltpu.SMEM((SCALES,), F32),
            pltpu.VMEM((SCALES, WIDTH), F32),
            pltpu.VMEM(block, F32),
            pltpu.VMEM((SLOTS, TILES, SCALES, 112, 128), BF16),
            pltpu.VMEM((SLOTS, WIDTH, WIDTH), F32),
            pltpu.VMEM((TILES, 104, 128), F32),
            pltpu.VMEM((128, WIDTH), F32),
            pltpu.VMEM((WIDTH, WIDTH), BF16),
            pltpu.VMEM((SLOTS, DEVS, 4, 128), F32),
            pltpu.VMEM((SLOTS, DEVS, 4, 128), F32),
            pltpu.VMEM((SLOTS - 1, 2 * DEVS, HALF), BF16),
            pltpu.VMEM((SLOTS - 1, 2 * DEVS, HALF), BF16),
            pltpu.SemaphoreType.DMA((5,)),
            pltpu.SemaphoreType.DMA((2, SLOTS)),
            pltpu.SemaphoreType.DMA((SLOTS,)),
            pltpu.SemaphoreType.DMA((len(GROUPS),)),
            pltpu.SemaphoreType.DMA((len(GROUPS),)),
        ],
        compiler_params=pltpu.CompilerParams(collective_id=0, has_side_effects=True, vmem_limit_bytes=44 * 2**20),
    )(*(pltpu.with_memory_space_constraint(v, pltpu.HBM) for v in (lat_order, wavenumber_of_slot, decay, amplitude, old, fresh, legendre)))
    new, pattern = pl.pallas_call(
        finish_kernel,
        name="finish",
        out_shape=(
            jax.ShapeDtypeStruct((SLOTS, SCALES, MEMBERS, 2, WIDTH), F32),
            jax.ShapeDtypeStruct((ROWS, MEMBERS, LON), F32),
        ),
        in_specs=[vmem] * 6,
        out_specs=(hbm, hbm),
        scratch_shapes=[
            pltpu.VMEM((ROWS, MEMBERS, LON), F32),
            pltpu.SemaphoreType.DMA((SLOTS,)),
            pltpu.SemaphoreType.DMA((ROWS,)),
        ],
        compiler_params=pltpu.CompilerParams(vmem_limit_bytes=24 * 2**20),
    )(*kept)
    return new.transpose(0, 3, 1, 2, 4), pattern


def solution(mesh):
    split_slots = P(("lat", "lon"), None, None, None, None)
    in_specs = (split_slots, split_slots, P(("lat", "lon"), None, None), P(), P(), P(), P())
    out_specs = (split_slots, P(("lat", "lon"), None, None))
    return jax.shard_map(local, mesh=mesh, in_specs=in_specs, out_specs=out_specs, check_vma=False)
```
